32 devices in a mesh: pod: 2 (over x), dp: 4 (over z), tp: 4 (over y, core).
Axes of the slice: x: 2, y: 2, z: 4, core: 2. Of those that a mesh axis runs over, the one named last changes fastest.
Arguments:
- x_in: bfloat16 [128, 512, 768], P(('pod', 'dp')), parts along dimension 0
- seg_ids: int32 [128, 512], P(('pod', 'dp')), parts along dimension 0
- gain_one: bfloat16 [768], replicated
- gain_two: bfloat16 [768], replicated
- w_qkv: bfloat16 [768, 2304], P(None, 'tp')
- w_out: bfloat16 [12, 64, 768], P('tp')
- w_up: bfloat16 [768, 3072], P(None, 'tp')
- w_down: bfloat16 [3072, 768], P('tp')
- grad_y: bfloat16 [128, 512, 768], P(('pod', 'dp')), parts along dimension 0
Outputs:
- output 1: bfloat16 [128, 512, 768], P(('pod', 'dp')), parts along dimension 0
- output 2: bfloat16 [128, 512, 768], P(('pod', 'dp')), parts along dimension 0
- output 3: bfloat16 [1536], P('pod'), parts along dimension 0
- output 4: bfloat16 [1536], P('pod'), parts along dimension 0
- output 5: bfloat16 [1536, 2304], P('pod', 'tp'), parts along dimension 0
- output 6: bfloat16 [24, 64, 768], P(('pod', 'tp')), parts along dimension 0
- output 7: bfloat16 [1536, 3072], P('pod', 'tp'), parts along dimension 0
- output 8: bfloat16 [6144, 768], P(('pod', 'tp')), parts along dimension 0
There are 2 independent parts. The reference program is written for one: setup_inputs(seed, part) draws one part's arguments, and reference() takes and returns one part's arrays. A program takes and returns all parts, laid end to end along the dimension named above; an argument that names none is the same for every part.
All inputs are finite; a program needn't handle non-finite values.
Results may differ from the reference program's by a relative error of at most 0.0189522.
Values are sent between devices in bfloat16 or wider.
A program may use at most 1 GiB of HBM per device.

```python
import functools
import jax
import jax.numpy as jnp
from jax import lax

BATCH_ROWS = 64
SEQ_LEN = 512
HIDDEN_DIM = 768
NUM_HEADS = 12
HEAD_DIM = 64
FFN_DIM = 3072
EPS_NORM = 1e-5


def setup_inputs(seed: int = 0, part: int = 0) -> dict:
    own_key = jax.random.fold_in(jax.random.key(seed), part)
    own_keys = jax.random.split(own_key, 3)
    shared_keys = jax.random.split(jax.random.key(seed + 1), 5)
    x_in = jax.random.normal(own_keys[0], (BATCH_ROWS, SEQ_LEN, HIDDEN_DIM), jnp.float32)
    cut_points = jax.random.randint(own_keys[1], (BATCH_ROWS, 3), 1, SEQ_LEN)
    positions = jnp.arange(SEQ_LEN)
    seg_ids = jnp.sum((positions[None, :, None] >= cut_points[:, None, :]).astype(jnp.int32), axis=-1)
    grad_y = jax.random.normal(own_keys[2], (BATCH_ROWS, SEQ_LEN, HIDDEN_DIM), jnp.float32)
    gain_pair = 1.0 + 0.3 * jax.random.normal(shared_keys[0], (2, HIDDEN_DIM), jnp.float32)
    qk_boost = jnp.array([1.5, 1.5, 1.0], jnp.float32)[None, None, :, None]
    w_qkv = jax.random.normal(shared_keys[1], (HIDDEN_DIM, NUM_HEADS, 3, HEAD_DIM), jnp.float32) * qk_boost * HIDDEN_DIM ** -0.5
    w_out = jax.random.normal(shared_keys[2], (NUM_HEADS, HEAD_DIM, HIDDEN_DIM), jnp.float32) * (2.0 * (NUM_HEADS * HEAD_DIM) ** -0.5)
    w_up = jax.random.normal(shared_keys[3], (HIDDEN_DIM, FFN_DIM), jnp.float32) * HIDDEN_DIM ** -0.5
    w_down = jax.random.normal(shared_keys[4], (FFN_DIM, HIDDEN_DIM), jnp.float32) * FFN_DIM ** -0.5
    return {
        "x_in": x_in.astype(jnp.bfloat16),
        "seg_ids": seg_ids,
        "gain_one": gain_pair[0].astype(jnp.bfloat16),
        "gain_two": gain_pair[1].astype(jnp.bfloat16),
        "w_qkv": w_qkv.reshape(HIDDEN_DIM, 3 * NUM_HEADS * HEAD_DIM).astype(jnp.bfloat16),
        "w_out": w_out.astype(jnp.bfloat16),
        "w_up": w_up.astype(jnp.bfloat16),
        "w_down": w_down.astype(jnp.bfloat16),
        "grad_y": grad_y.astype(jnp.bfloat16),
    }


def layer_norm(x_rows, gain_vec):
    x_f32 = x_rows.astype(jnp.float32)
    centered = x_f32 - jnp.mean(x_f32, axis=-1, keepdims=True)
    variance = jnp.mean(centered * centered, axis=-1, keepdims=True)
    return (centered * lax.rsqrt(variance + EPS_NORM) * gain_vec.astype(jnp.float32)).astype(jnp.bfloat16)


def head_attention(qkv_item, seg_row):
    scores = jnp.dot(qkv_item[0], qkv_item[1].T, preferred_element_type=jnp.float32) * (HEAD_DIM ** -0.5)
    positions = jnp.arange(SEQ_LEN)
    allowed = (positions[:, None] >= positions[None, :]) & (seg_row[:, None] == seg_row[None, :])
    attn_probs = jax.nn.softmax(jnp.where(allowed, scores, -1e30), axis=-1)
    return jnp.dot(attn_probs.astype(jnp.bfloat16), qkv_item[2], preferred_element_type=jnp.float32).astype(jnp.bfloat16)


def layer_forward(seg_ids, x_in, gain_one, gain_two, w_qkv, w_out, w_up, w_down):
    tokens = BATCH_ROWS * SEQ_LEN
    x_rows = x_in.reshape(tokens, HIDDEN_DIM)
    normed_a = layer_norm(x_rows, gain_one)
    qkv_rows = jnp.dot(normed_a, w_qkv, preferred_element_type=jnp.float32).astype(jnp.bfloat16)
    qkv_rows = qkv_rows.reshape(BATCH_ROWS, SEQ_LEN, NUM_HEADS, 3, HEAD_DIM)
    qkv_rows = jnp.transpose(qkv_rows, (0, 2, 3, 1, 4)).reshape(BATCH_ROWS * NUM_HEADS, 3, SEQ_LEN, HEAD_DIM)
    seg_rep = jnp.repeat(seg_ids, NUM_HEADS, axis=0)
    attn_out = lax.map(lambda map_item: jax.checkpoint(head_attention)(map_item[0], map_item[1]), (qkv_rows, seg_rep))
    attn_out = jnp.transpose(attn_out.reshape(BATCH_ROWS, NUM_HEADS, SEQ_LEN, HEAD_DIM), (0, 2, 1, 3)).reshape(tokens, NUM_HEADS * HEAD_DIM)
    part_one = jnp.dot(attn_out, w_out.reshape(NUM_HEADS * HEAD_DIM, HIDDEN_DIM), preferred_element_type=jnp.float32).astype(jnp.bfloat16)
    x_one = (x_rows.astype(jnp.float32) + part_one.astype(jnp.float32)).astype(jnp.bfloat16)
    normed_b = layer_norm(x_one, gain_two)
    pre_act = jnp.dot(normed_b, w_up, preferred_element_type=jnp.float32)
    hidden_act = jax.nn.gelu(pre_act, approximate=True).astype(jnp.bfloat16)
    part_two = jnp.dot(hidden_act, w_down, preferred_element_type=jnp.float32).astype(jnp.bfloat16)
    y_rows = (x_one.astype(jnp.float32) + part_two.astype(jnp.float32)).astype(jnp.bfloat16)
    return y_rows.reshape(BATCH_ROWS, SEQ_LEN, HIDDEN_DIM)


def reference(x_in, seg_ids, gain_one, gain_two, w_qkv, w_out, w_up, w_down, grad_y):
    y_out, pullback = jax.vjp(functools.partial(layer_forward, seg_ids), x_in, gain_one, gain_two, w_qkv, w_out, w_up, w_down)
    grad_list = pullback(grad_y)
    return (y_out, grad_list[0], grad_list[1], grad_list[2], grad_list[3], grad_list[4], grad_list[5], grad_list[6])
```

```python
import functools

import jax
import jax.numpy as jnp
from jax import lax
from jax.experimental import pallas as pl
from jax.experimental.pallas import tpu as pltpu
from jax.sharding import PartitionSpec as P


EPS_NORM = 1e-5
MASKED = -1e30
OPEN = 3e38
LOG2E = 1.4426950408889634
NT = (((1,), (1,)), ((), ()))
TN = (((0,), (0,)), ((), ()))
NN = (((1,), (0,)), ((), ()))
HEADS_PER_STEP = 2
PLACE_ROWS = 512
GAIN_ROWS = 64


def dot32(lhs, rhs, dims):
    return lax.dot_general(lhs, rhs, dims, preferred_element_type=jnp.float32)


def norm_forward(x_rows, gain_vec):
    x_f32 = x_rows.astype(jnp.float32)
    centered = x_f32 - jnp.mean(x_f32, axis=-1, keepdims=True)
    inv_std = lax.rsqrt(jnp.mean(centered * centered, axis=-1, keepdims=True) + EPS_NORM)
    x_hat = centered * inv_std
    return (x_hat * gain_vec.astype(jnp.float32)).astype(jnp.bfloat16), x_hat, inv_std


def norm_backward(grad_out, x_hat, inv_std, gain_vec):
    grad_f32 = grad_out.astype(jnp.float32)
    grad_gain = jnp.sum(grad_f32 * x_hat, axis=0)
    grad_hat = grad_f32 * gain_vec.astype(jnp.float32)
    mean_one = jnp.mean(grad_hat, axis=-1, keepdims=True)
    mean_two = jnp.mean(grad_hat * x_hat, axis=-1, keepdims=True)
    return inv_std * (grad_hat - mean_one - x_hat * mean_two), grad_gain


def fill_limit(seg_q_ref, seg_k_ref, limit_ref):
    seq = limit_ref.shape[0]
    key_pos = lax.broadcasted_iota(jnp.int32, (seq, seq), 0)
    query_pos = lax.broadcasted_iota(jnp.int32, (seq, seq), 1)
    allowed = (key_pos <= query_pos) & (seg_k_ref[0] == seg_q_ref[0])
    limit_ref[...] = jnp.where(allowed, OPEN, MASKED)


def attn_fwd_kernel(head_dim, score_scale, seg_q_ref, seg_k_ref, qkv_ref, out_ref, lse_ref, limit_ref):
    @pl.when(pl.program_id(1) == 0)
    def _():
        fill_limit(seg_q_ref, seg_k_ref, limit_ref)

    seq = limit_ref.shape[0]
    half = seq // 2
    factor = score_scale * LOG2E
    for head in range(HEADS_PER_STEP):
        base = head * 3 * head_dim
        q_t = qkv_ref[base : base + head_dim, :]
        k_t = qkv_ref[base + head_dim : base + 2 * head_dim, :]
        v_t = qkv_ref[base + 2 * head_dim : base + 3 * head_dim, :]
        for blk in range(2):
            keys = (blk + 1) * half
            cols = slice(blk * half, (blk + 1) * half)
            raw = dot32(k_t[:, :keys], q_t[:, cols], TN)
            raw = jnp.minimum(raw, limit_ref[:keys, cols])
            top = jnp.max(raw, axis=0, keepdims=True)
            weights = jnp.exp2((raw - top) * factor)
            total = jnp.sum(weights, axis=0, keepdims=True)
            out = dot32(v_t[:, :keys], weights.astype(jnp.bfloat16), NN)
            out_ref[head * head_dim : (head + 1) * head_dim, cols] = (out / total).astype(jnp.bfloat16)
            lse_ref[0, 0, head : head + 1, cols] = top * factor + jnp.log2(total)


def attn_bwd_kernel(head_dim, score_scale, seg_q_ref, seg_k_ref, qkv_ref, out_ref, lse_ref, grad_ref, dqkv_ref, limit_ref):
    @pl.when(pl.program_id(1) == 0)
    def _():
        fill_limit(seg_q_ref, seg_k_ref, limit_ref)

    seq = limit_ref.shape[0]
    half = seq // 2
    factor = score_scale * LOG2E
    for head in range(HEADS_PER_STEP):
        base = head * 3 * head_dim
        q_t = qkv_ref[base : base + head_dim, :]
        k_t = qkv_ref[base + head_dim : base + 2 * head_dim, :]
        v_t = qkv_ref[base + 2 * head_dim : base + 3 * head_dim, :]
        g_t = grad_ref[head * head_dim : (head + 1) * head_dim, :]
        o_t = out_ref[head * head_dim : (head + 1) * head_dim, :]
        delta = jnp.sum(g_t.astype(jnp.float32) * o_t.astype(jnp.float32), axis=0, keepdims=True)
        grads_k, grads_v = [], []
        for blk in range(2):
            keys = (blk + 1) * half
            cols = slice(blk * half, (blk + 1) * half)
            raw = dot32(k_t[:, :keys], q_t[:, cols], TN)
            raw = jnp.minimum(raw, limit_ref[:keys, cols])
            probs = jnp.exp2(raw * factor - lse_ref[0, 0, head : head + 1, cols])
            grad_p = dot32(v_t[:, :keys], g_t[:, cols], TN)
            grad_s = (probs * (grad_p - delta[:, cols])).astype(jnp.bfloat16)
            grads_v.append(dot32(g_t[:, cols], probs.astype(jnp.bfloat16), NT))
            grads_k.append(dot32(q_t[:, cols], grad_s, NT))
            grad_q = dot32(k_t[:, :keys], grad_s, NN) * score_scale
            dqkv_ref[base : base + head_dim, cols] = grad_q.astype(jnp.bfloat16)
        for pos, (low, full) in enumerate((grads_k, grads_v)):
            scale = score_scale if pos == 0 else 1.0
            start = base + (pos + 1) * head_dim
            dqkv_ref[start : start + head_dim, :half] = ((low + full[:, :half]) * scale).astype(jnp.bfloat16)
            dqkv_ref[start : start + head_dim, half:] = (full[:, half:] * scale).astype(jnp.bfloat16)


def attn_specs(head_dim, seq):
    step_rows = HEADS_PER_STEP * head_dim
    return {
        "seg_q": pl.BlockSpec((1, 1, seq), lambda b, h: (b, 0, 0)),
        "seg_k": pl.BlockSpec((1, seq, 1), lambda b, h: (b, 0, 0)),
        "qkv": pl.BlockSpec((3 * step_rows, seq), lambda b, h: (h, b)),
        "out": pl.BlockSpec((step_rows, seq), lambda b, h: (h, b)),
        "lse": pl.BlockSpec((1, 1, HEADS_PER_STEP, seq), lambda b, h: (b, h, 0, 0)),
    }


def attention_forward(seg_q, seg_k, qkv_t, batch, heads, head_dim, seq):
    specs = attn_specs(head_dim, seq)
    groups = heads // HEADS_PER_STEP
    return pl.pallas_call(
        functools.partial(attn_fwd_kernel, head_dim, head_dim ** -0.5),
        grid=(batch, groups),
        in_specs=[specs["seg_q"], specs["seg_k"], specs["qkv"]],
        out_specs=[specs["out"], specs["lse"]],
        out_shape=[
            jax.ShapeDtypeStruct((heads * head_dim, batch * seq), jnp.bfloat16),
            jax.ShapeDtypeStruct((batch, groups, HEADS_PER_STEP, seq), jnp.float32),
        ],
        scratch_shapes=[pltpu.VMEM((seq, seq), jnp.float32)],
        cost_estimate=pl.CostEstimate(flops=batch * heads * seq * seq * head_dim * 16, bytes_accessed=12 << 20, transcendentals=batch * heads * seq * seq),
        name="attn_fwd",
    )(seg_q, seg_k, qkv_t)


def attention_backward(seg_q, seg_k, qkv_t, out_t, lse, grad_t, batch, heads, head_dim, seq):
    specs = attn_specs(head_dim, seq)
    return pl.pallas_call(
        functools.partial(attn_bwd_kernel, head_dim, head_dim ** -0.5),
        grid=(batch, heads // HEADS_PER_STEP),
        in_specs=[specs["seg_q"], specs["seg_k"], specs["qkv"], specs["out"], specs["lse"], specs["out"]],
        out_specs=specs["qkv"],
        out_shape=jax.ShapeDtypeStruct((3 * heads * head_dim, batch * seq), jnp.bfloat16),
        scratch_shapes=[pltpu.VMEM((seq, seq), jnp.float32)],
        cost_estimate=pl.CostEstimate(flops=batch * heads * seq * seq * head_dim * 40, bytes_accessed=24 << 20, transcendentals=batch * heads * seq * seq),
        name="attn_bwd",
    )(seg_q, seg_k, qkv_t, out_t, lse, grad_t)


def place_kernel(slots_ref, one_ref, two_ref, *rest):
    out_ref = rest[-1]

    @pl.when(pl.program_id(0) == 0)
    def _():
        out_ref[0] = one_ref[...]

    @pl.when(pl.program_id(0) == 1)
    def _():
        out_ref[0] = two_ref[...]


def place_pair(slots, one, two, slot_count, base=None):
    rows, width = one.shape
    chunks = rows // PLACE_ROWS
    last = chunks - 1
    block = (PLACE_ROWS, width)
    in_specs = [
        pl.BlockSpec(block, lambda s, c, slots: (jnp.where(s == 0, c, last), 0)),
        pl.BlockSpec(block, lambda s, c, slots: (jnp.where(s == 0, 0, c), 0)),
    ]
    operands = [slots, one, two]
    aliases = {}
    if base is not None:
        in_specs.append(pl.BlockSpec(memory_space=pl.ANY))
        operands.append(base)
        aliases = {3: 0}
    return pl.pallas_call(
        place_kernel,
        grid_spec=pltpu.PrefetchScalarGridSpec(
            num_scalar_prefetch=1,
            grid=(2, chunks),
            in_specs=in_specs,
            out_specs=pl.BlockSpec((1,) + block, lambda s, c, slots: (slots[s], c, 0)),
        ),
        out_shape=jax.ShapeDtypeStruct((slot_count, rows, width), one.dtype),
        input_output_aliases=aliases,
        cost_estimate=pl.CostEstimate(flops=0, bytes_accessed=4 * rows * width * 2, transcendentals=0),
        name="place_pair",
    )(*operands)


def add_low(*parts):
    total = parts[0].astype(jnp.float32)
    for part in parts[1:]:
        total = total + part.astype(jnp.float32)
    return total.astype(jnp.bfloat16)


def ring_sum(mat, axis, size):
    rows = mat.shape[0] // size
    half = rows // 32 * 16
    me = lax.axis_index(axis)
    upward = [(i, (i + 1) % size) for i in range(size)]
    downward = [(i, (i - 1) % size) for i in range(size)]
    chunks = mat.reshape(size, rows, mat.shape[1])
    own, following, opposite, previous = (
        lax.dynamic_index_in_dim(chunks, lax.rem(me + k, size), 0, keepdims=False) for k in range(size)
    )
    low = lax.ppermute(opposite[:half], axis, upward)
    high = lax.ppermute(opposite[half:], axis, downward)
    to_next = jnp.concatenate([add_low(following[:half], low), following[half:]])
    to_previous = jnp.concatenate([previous[:half], add_low(previous[half:], high)])
    from_previous = lax.ppermute(to_next, axis, upward)
    from_next = lax.ppermute(to_previous, axis, downward)
    total = add_low(own, from_previous, from_next)
    have_previous = lax.ppermute(total, axis, upward)
    have_next = lax.ppermute(total, axis, downward)
    far_low = lax.ppermute(have_previous[:half], axis, upward)
    far_high = lax.ppermute(have_next[half:], axis, downward)
    whole = jnp.zeros_like(mat)
    far_row = lax.rem(me + 2, size) * rows
    for block, row in (
        (total, me * rows),
        (have_next, lax.rem(me + 1, size) * rows),
        (have_previous, lax.rem(me + size - 1, size) * rows),
        (far_low, far_row),
        (far_high, far_row + half),
    ):
        whole = lax.dynamic_update_slice_in_dim(whole, block, row, 0)
    return whole


def gelu_tanh(values):
    return jax.nn.gelu(values, approximate=True)


def solution(mesh):
    tp_size = mesh.shape["tp"]
    dp_size = mesh.shape["dp"]
    batch_spec = P(("pod", "dp"), None, None)
    seg_spec = P(("pod", "dp"), None)
    far_pairs = [(i, i ^ 2) for i in range(tp_size)]
    near_pairs = [(i, i ^ 1) for i in range(tp_size)]
    hold = lax.optimization_barrier

    def local_step(x_in, seg_ids, gain_one, gain_two, w_qkv, w_out, w_up, w_down, grad_y):
        batch_loc, seq, hidden = x_in.shape
        heads = w_out.shape[0] * tp_size
        head_dim = w_out.shape[1]
        batch = batch_loc // tp_size
        tokens = batch * seq
        me = lax.axis_index("tp")
        first = me * batch

        def gather(mat):
            return lax.all_gather(mat, "tp", axis=0, tiled=True)

        def scatter(mat):
            return lax.psum_scatter(mat, "tp", scatter_dimension=0, tiled=True)

        def exchange(rows):
            far = lax.ppermute(rows, "tp", far_pairs)
            near = lax.ppermute(rows, "tp", near_pairs)
            far_near = lax.ppermute(far, "tp", near_pairs)
            return near, far, far_near

        def assemble(rows, parts):
            near, far, far_near = parts
            half = place_pair(jnp.stack([me, me ^ 1]), rows, near, tp_size)
            whole = place_pair(jnp.stack([me ^ 2, me ^ 3]), far, far_near, tp_size, half)
            return whole.reshape(x_in.shape)

        wqkv_t = gather(w_qkv.T)
        wout = gather(w_out.reshape(-1, hidden))
        wup_t = gather(w_up.T)
        wdown = gather(w_down)

        x_rows = lax.dynamic_slice_in_dim(x_in, first, batch, 0).reshape(tokens, hidden)
        grad_rows = lax.dynamic_slice_in_dim(grad_y, first, batch, 0).reshape(tokens, hidden)
        seg = lax.dynamic_slice_in_dim(seg_ids, first, batch, 0)
        seg_q, seg_k = seg[:, None, :], seg[:, :, None]

        normed_a, hat_a, inv_a = norm_forward(x_rows, gain_one)
        qkv_t = dot32(wqkv_t, normed_a, NT).astype(jnp.bfloat16)
        out_t, lse = attention_forward(seg_q, seg_k, qkv_t, batch, heads, head_dim, seq)
        part_one = dot32(out_t, wout, TN).astype(jnp.bfloat16)
        x_one = (x_rows.astype(jnp.float32) + part_one.astype(jnp.float32)).astype(jnp.bfloat16)
        normed_b, hat_b, inv_b = norm_forward(x_one, gain_two)
        normed_b = hold(normed_b)
        pre_act = dot32(normed_b, wup_t, NT)
        act_val, gelu_pull = jax.vjp(gelu_tanh, pre_act)
        hidden_act = hold(act_val.astype(jnp.bfloat16))
        part_two = dot32(hidden_act, wdown, NN).astype(jnp.bfloat16)
        y_rows = (x_one.astype(jnp.float32) + part_two.astype(jnp.float32)).astype(jnp.bfloat16)
        y_rows, hidden_act, grad_rows = hold((y_rows, hidden_act, grad_rows))
        y_parts = exchange(y_rows)

        grad_down = dot32(hidden_act, grad_rows, TN).astype(jnp.bfloat16)
        grad_down, grad_rows = hold((grad_down, grad_rows))
        red_down = scatter(grad_down)
        grad_hidden = dot32(grad_rows, wdown, NT).astype(jnp.bfloat16)
        grad_pre = gelu_pull(grad_hidden.astype(jnp.float32))[0].astype(jnp.bfloat16)
        grad_up_t = dot32(grad_pre, normed_b, TN).astype(jnp.bfloat16)
        grad_up_t, grad_pre = hold((grad_up_t, grad_pre))
        red_up_t = scatter(grad_up_t)
        grad_norm_b = dot32(grad_pre, wup_t, NN).astype(jnp.bfloat16)
        back_b, gain_grad_two = norm_backward(grad_norm_b, hat_b, inv_b, gain_two)
        grad_x_one = (grad_rows.astype(jnp.float32) + back_b).astype(jnp.bfloat16)
        grad_out_w = dot32(out_t, grad_x_one, NN).astype(jnp.bfloat16)
        grad_out_w, grad_x_one = hold((grad_out_w, grad_x_one))
        red_out = scatter(grad_out_w)
        grad_attn_t = dot32(wout, grad_x_one, NT).astype(jnp.bfloat16)
        grad_qkv_t = attention_backward(seg_q, seg_k, qkv_t, out_t, lse, grad_attn_t, batch, heads, head_dim, seq)
        grad_norm_a = dot32(grad_qkv_t, wqkv_t, TN).astype(jnp.bfloat16)
        back_a, gain_grad_one = norm_backward(grad_norm_a, hat_a, inv_a, gain_one)
        grad_x = (grad_x_one.astype(jnp.float32) + back_a).astype(jnp.bfloat16)
        grad_x, grad_qkv_t = hold((grad_x, grad_qkv_t))
        grad_x_parts = exchange(grad_x)

        grad_wqkv_t = dot32(grad_qkv_t, normed_a, NN).astype(jnp.bfloat16)
        gains = jnp.stack([gain_grad_one, gain_grad_two]).astype(jnp.bfloat16)
        gains = jnp.pad(gains, ((0, GAIN_ROWS - 2), (0, 0)))
        packed = jnp.concatenate(
            [grad_wqkv_t.reshape(tp_size, -1, hidden), jnp.broadcast_to(gains, (tp_size,) + gains.shape)], axis=1
        ).reshape(-1, hidden)
        packed, red_down, red_up_t, red_out = hold((packed, red_down, red_up_t, red_out))
        red_packed = scatter(packed)
        sum_first = ring_sum(jnp.concatenate([red_down, red_up_t, red_out]), "dp", dp_size)
        sum_packed = ring_sum(red_packed, "dp", dp_size)
        up_start = red_down.shape[0]
        out_start = up_start + red_up_t.shape[0]
        sum_down, sum_up_t, sum_out = sum_first[:up_start], sum_first[up_start:out_start], sum_first[out_start:]
        qkv_rows = w_qkv.shape[1]

        y_full = assemble(y_rows, y_parts)
        grad_x_full = assemble(grad_x, grad_x_parts)
        return (
            y_full,
            grad_x_full,
            sum_packed[qkv_rows],
            sum_packed[qkv_rows + 1],
            sum_packed[:qkv_rows].T,
            sum_out.reshape(w_out.shape),
            sum_up_t.T,
            sum_down,
        )

    return jax.shard_map(
        local_step,
        mesh=mesh,
        in_specs=(batch_spec, seg_spec, P(None), P(None), P(None, "tp"), P("tp", None, None), P(None, "tp"), P("tp", None), batch_spec),
        out_specs=(batch_spec, batch_spec, P("pod"), P("pod"), P("pod", "tp"), P(("pod", "tp"), None, None), P("pod", "tp"), P(("pod", "tp"), None)),
        check_vma=False,
    )
```
